32 devices in a mesh: gx: 4 (over y, core), gy: 8 (over z, x).
Axes of the slice: x: 2, y: 2, z: 4, core: 2. Of those that a mesh axis runs over, the one named last changes fastest.
Arguments:
- position: float32 [4, 8, 3, 4096], P('gx', 'gy'), may hold values from 0 to 8, as said below
- velocity: float32 [4, 8, 3, 4096], P('gx', 'gy'), may hold values from -6 to 6
- mass: float32 [4, 8, 1, 4096], P('gx', 'gy'), may hold values from 0.3 to 3
- pair_list: int32 [4, 8, 32, 27], P('gx', 'gy'), may hold values from 0 to 287, as said below
- hot_leaf: int32 [4, 8, 8], P('gx', 'gy'), may hold values from 0 to 32, as said below
Outputs:
- displacement: float32 [4, 8, 3, 4096], P('gx', 'gy')
- new_velocity: float32 [4, 8, 3, 4096], P('gx', 'gy')
The draws below stay inside these ranges and needn't reach their ends.
Inputs may be any that keep to these rules, and one draw needn't show every extreme that they name: `pair_list`: entry k of every list names a leaf of neighbourhood block k mod 9. `position`: component 0 of a particle of cell (i, j) lies in [i, i + 1), component 1 in [j, j + 1), component 2 in [0, 1). `hot_leaf`: the slots of a cell hold distinct leaf numbers first and the empty mark 32 after them; cell (i, j) and cell (i, (j + 4) mod 8) hold exactly 8 hot leaves together.
All inputs are finite; a program needn't handle non-finite values.
Results may differ from the reference program's by a relative error of at most 0.00023.
Values sent between devices are 32-bit elements; how exact they have to be, the bound alone decides.
A program may use at most 64 MiB of HBM per device.

```python
import math
import jax
import jax.numpy as jnp
from jax import lax

LEAF = 128
LEAF_DEV = 32
PAIRS = 27
HOT = 8
PART = 4096
NGX = 4
NGY = 8
N_GX = 4
N_GY = 8


def draw_position(key, part):
    shape = (N_GX, N_GY, 3, LEAF_DEV * LEAF)
    inside = jax.random.uniform(key, shape, jnp.float32)
    row_index = lax.broadcasted_iota(jnp.int32, shape, 0).astype(jnp.float32)
    column_index = lax.broadcasted_iota(jnp.int32, shape, 1).astype(jnp.float32)
    channel = lax.broadcasted_iota(jnp.int32, shape, 2)
    offset = jnp.where(channel == 0, row_index, 0.0) + jnp.where(channel == 1, column_index, 0.0)
    return inside + offset


def draw_pair_list(key, part):
    shape = (N_GX, N_GY, LEAF_DEV, PAIRS)
    chosen = jax.random.randint(key, shape, 0, LEAF_DEV, jnp.int32)
    block = lax.broadcasted_iota(jnp.int32, shape, 3) % 9
    return block * LEAF_DEV + chosen


def draw_hot_leaf(key, part):
    first_key = jax.random.fold_in(key, 11)
    second_key = jax.random.fold_in(key, 23)
    half = N_GY // 2
    lower = jax.random.randint(first_key, (N_GX, half), 0, HOT + 1, jnp.int32)
    counts = jnp.concatenate([lower, HOT - lower], axis=1)
    scores = jax.random.randint(second_key, (N_GX, N_GY, LEAF_DEV), 0, 1 << 20, jnp.int32)
    leaves = lax.broadcasted_iota(jnp.int32, (N_GX, N_GY, LEAF_DEV), 2)
    order = jnp.argsort(scores * LEAF_DEV + leaves, axis=-1).astype(jnp.int32)[:, :, :HOT]
    slots = lax.broadcasted_iota(jnp.int32, (N_GX, N_GY, HOT), 2)
    return jnp.where(slots < counts[:, :, None], order, LEAF_DEV).astype(jnp.int32)


def shard_levels(stream_key, dims, cuts, low, top_value):
    def one(dim, shards_of):
        draws = jax.random.uniform(jax.random.fold_in(jax.random.fold_in(stream_key, 6), dim), (shards_of,), jnp.float32, low / len(cuts), top_value / len(cuts))
        return jnp.repeat(jnp.exp(draws), dims[dim] // shards_of).reshape((-1,) + (1,) * (len(dims) - dim - 1))

    level = one(*cuts[0])
    for cut in cuts[1:]:
        level = level * one(*cut)
    return level


def normal_values(rng, shape, scale, limit, shards=(), kind=jnp.bfloat16):
    array = scale * jax.random.normal(rng, shape, jnp.float32)
    if shards:
        array = array * shard_levels(rng, shape, shards, -0.22, 0.18)
    return jnp.clip(array, -limit, limit).astype(kind)


def setup_inputs(seed: int = 0) -> dict:
    keys = jax.random.split(jax.random.key(seed), 6)
    return {
        "position": draw_position(jax.random.fold_in(keys[5], 71), 0),
        "velocity": normal_values(keys[1], (NGX, NGY, 3, PART), 1.0, 6.0, ((0, 4), (1, 8)), jnp.float32),
        "mass": jnp.clip(jnp.exp(math.log(3.0) - 2.3025851 * jax.random.uniform(keys[2], (NGX, NGY, 1, PART), jnp.float32) ** shard_levels(keys[2], (NGX, NGY, 1, PART), ((0, 4), (1, 8)), -0.2, 0.2)), 0.3, 3.0),
        "pair_list": draw_pair_list(jax.random.fold_in(keys[5], 71), 0),
        "hot_leaf": draw_hot_leaf(jax.random.fold_in(keys[5], 71), 0),
    }


kernel_scale = 1.0
viscosity = 0.5
time_step = 0.5
base_entries = 9


def source_leaves(extended):
    channels = extended.shape[2]
    count = extended.shape[3] // LEAF
    return jnp.transpose(extended, (2, 0, 1, 3)).reshape(channels, 9 * count, LEAF)


def own_leaves(own):
    channels = own.shape[0]
    count = own.shape[1] // LEAF
    return jnp.transpose(own.reshape(channels, count, LEAF), (1, 0, 2))


def inverse_density(own, extended, pairs, usage):
    sources = source_leaves(extended)

    def one_leaf(inputs):
        target, chosen, used = inputs
        picked = jnp.take(sources, chosen, axis=1)
        near_mass = (picked[6] * used[:, None]).reshape(-1)
        near = picked.reshape(sources.shape[0], -1)
        diff = target[0:3, :, None] - near[0:3, None, :]
        weight = jnp.exp(-jnp.sum(diff * diff, axis=0) / kernel_scale)
        rho = target[6] + jnp.sum(near_mass[None, :] * weight, axis=1)
        return 1.0 / rho

    result = lax.map(one_leaf, (own_leaves(own), pairs, usage))
    return result.reshape(1, -1)


def acceleration(own, own_inverse, extended, extended_inverse, pairs, usage):
    sources = source_leaves(extended)
    source_inverse = source_leaves(extended_inverse)[0]
    targets = own_leaves(own)
    target_inverse = own_inverse.reshape(-1, LEAF)

    def one_leaf(inputs):
        target, target_q, chosen, used = inputs
        picked = jnp.take(sources, chosen, axis=1)
        near_mass = (picked[6] * used[:, None]).reshape(-1)
        near = picked.reshape(sources.shape[0], -1)
        near_q = jnp.take(source_inverse, chosen, axis=0).reshape(-1)
        diff = target[0:3, :, None] - near[0:3, None, :]
        weight = jnp.exp(-jnp.sum(diff * diff, axis=0) / kernel_scale)
        massed = near_mass[None, :] * weight
        press = massed * (2.0 / kernel_scale) * (target_q[:, None] + near_q[None, :])
        pushed = jnp.sum(press[None] * diff, axis=2)
        damped = jnp.sum((massed * near_q[None, :])[None] * (near[3:6, None, :] - target[3:6, :, None]), axis=2)
        return pushed + viscosity * damped

    result = lax.map(one_leaf, (targets, target_inverse, pairs, usage))
    return jnp.transpose(result, (1, 0, 2)).reshape(3, -1)


def neighbourhood(field):
    rows, columns = field.shape[0], field.shape[1]
    padded = jnp.pad(field, ((1, 1), (1, 1), (0, 0), (0, 0)))
    blocks = jnp.stack([jnp.stack([padded[a:a + rows, b:b + columns] for b in range(3)], axis=2) for a in range(3)], axis=2)
    return blocks.reshape((rows * columns, 3, 3) + field.shape[2:])


def entry_usage(flat_hot):
    leaves = jnp.arange(LEAF_DEV, dtype=jnp.int32)
    is_hot = jnp.any(flat_hot[:, :, None] == leaves[None, None, :], axis=1)
    entries = jnp.arange(PAIRS, dtype=jnp.int32)
    used = (entries[None, None, :] < base_entries) | is_hot[:, :, None]
    return jnp.where(used, 1.0, 0.0).astype(jnp.float32)


def section_all(position, velocity, mass, pair_list, hot_leaf):
    rows, columns = position.shape[0], position.shape[1]
    own = jnp.concatenate([position, velocity, mass], axis=2)
    flat_own = own.reshape((rows * columns,) + own.shape[2:])
    flat_pairs = pair_list.reshape((rows * columns,) + pair_list.shape[2:])
    usage = entry_usage(hot_leaf.reshape(rows * columns, -1))
    extended = neighbourhood(own)
    inverse = lax.map(lambda z: inverse_density(z[0], z[1], z[2], z[3]), (flat_own, extended, flat_pairs, usage))
    extended_inverse = neighbourhood(inverse.reshape(rows, columns, 1, -1))
    acc = lax.map(lambda z: acceleration(z[0], z[1], z[2], z[3], z[4], z[5]), (flat_own, inverse, extended, extended_inverse, flat_pairs, usage))
    return acc.reshape(position.shape)


def reference(position, velocity, mass, pair_list, hot_leaf):
    first = section_all(position, velocity, mass, pair_list, hot_leaf)
    mid_position = position + 0.5 * time_step * velocity
    mid_velocity = velocity + 0.5 * time_step * first
    second = section_all(mid_position, mid_velocity, mass, pair_list, hot_leaf)
    return time_step * mid_velocity, velocity + time_step * second
```

```python
import functools

import jax
import jax.numpy as jnp
from jax import lax
from jax.experimental import pallas as pl
from jax.experimental.pallas import tpu as pltpu
from jax.sharding import PartitionSpec as P

LEAF = 128

kernel_scale = 1.0
viscosity = 0.5
time_step = 0.5
base_entries = 9
COORD = (2.0 * 1.4426950408889634 / kernel_scale) ** 0.5


def with_halo(cells, sides, width):
    for axis, dim in sides:
        count = lax.axis_size(axis)
        ends = count - 1
        head = lax.slice_in_dim(cells, 0, width, axis=dim)
        tail = lax.slice_in_dim(cells, cells.shape[dim] - width, cells.shape[dim], axis=dim)
        cells = jnp.concatenate(
            [
                lax.ppermute(tail, axis, [(i, (i + 1) % count) for i in range(ends)]),
                cells,
                lax.ppermute(head, axis, [((i + 1) % count, i) for i in range(ends)]),
            ],
            axis=dim,
        )
    return cells


def surround(cell):
    extended = with_halo(cell, (("gx", 0), ("gy", 1)), 1)
    return extended.reshape((9,) + extended.shape[2:])


def split3(value):
    first = value.astype(jnp.bfloat16).astype(jnp.float32)
    rest = value - first
    second = rest.astype(jnp.bfloat16).astype(jnp.float32)
    third = (rest - second).astype(jnp.bfloat16).astype(jnp.float32)
    return first, second, third


def coordinate_rows(x, ones_first):
    a = COORD * x
    c = -0.5 * jnp.sum(a * a, axis=0, keepdims=True)
    one = jnp.ones_like(c)
    pad = jnp.zeros_like(a)
    return jnp.concatenate([a, one, c, pad] if ones_first else [a, c, one, pad], axis=0)


def pair_sums(sections, counts, src_ref, leaf_ref, live_ref, *refs):
    place_refs, channel_refs = refs[:sections], refs[sections : 2 * sections]
    out_refs = refs[2 * sections : 3 * sections]
    feature, target, channel = refs[3 * sections :]
    base_items, entries = counts
    blocks, _, width = place_refs[0].shape
    step = min(width, 8 * LEAF)
    own = blocks // 2
    for place_ref, channel_ref, out_ref in zip(place_refs, channel_refs, out_refs):
        for block in range(blocks):

            def prepare(i, carry):
                span = pl.ds(pl.multiple_of(i * step, step), step)
                rows = coordinate_rows(place_ref[block, 0:3, span], True)
                s1, s2, s3 = split3(rows)
                feature[block, :, span] = jnp.concatenate(
                    [s1, s2, s1, s2, s3, s1], axis=0
                ).astype(jnp.bfloat16)
                c1, c2, _ = split3(channel_ref[block, :, span])
                channel[block, :, span] = jnp.concatenate([c1, c2], axis=0).astype(jnp.bfloat16)
                return carry

            lax.fori_loop(0, width // step, prepare, 0)

        def prepare_target(i, carry):
            span = pl.ds(pl.multiple_of(i * LEAF, LEAF), LEAF)
            rows = coordinate_rows(place_ref[own, 0:3, span], False)
            t1, t2, t3 = split3(rows)
            stack = jnp.concatenate(
                [t1, t1, t2, t2, t1, t3, jnp.zeros((LEAF - 48, LEAF), jnp.float32)], axis=0
            )
            target[i] = stack.T.astype(jnp.bfloat16)
            return carry

        lax.fori_loop(0, width // LEAF, prepare_target, 0)

        def sums(item):
            leaf = leaf_ref[item]
            spans = [
                pl.ds(pl.multiple_of(src_ref[item * entries + k] * LEAF, LEAF), LEAF)
                for k in range(entries)
            ]
            near = jnp.concatenate([feature[k, :, spans[k]] for k in range(entries)], axis=1)
            exponent = jnp.dot(
                target[leaf][:, 0:48], near, preferred_element_type=jnp.float32
            )
            weight = jnp.exp2(exponent).astype(jnp.bfloat16)
            rows = jnp.concatenate([channel[k, :, spans[k]] for k in range(entries)], axis=1)
            both = lax.dot_general(
                rows, weight, (((1,), (1,)), ((), ())), preferred_element_type=jnp.float32
            )
            return leaf, both[0:8] + both[8:16]

        def base(i, carry):
            for u in range(4):
                leaf, value = sums(i * 4 + u)
                out_ref[leaf] = value
            return carry

        lax.fori_loop(0, base_items // 4, base, 0)

        def extra(i, carry):
            leaf, first = sums(base_items + 2 * i)
            _, second = sums(base_items + 2 * i + 1)
            out_ref[leaf] = out_ref[leaf] + (first + second)
            return carry

        lax.fori_loop(0, live_ref[0], extra, 0)


def all_sums(tables, places, channels):
    src, leaves, live, base_items = tables
    sections = len(places)
    blocks, _, width = places[0].shape
    count = width // LEAF
    smem = pl.BlockSpec(memory_space=pltpu.SMEM)
    vmem = pl.BlockSpec(memory_space=pltpu.VMEM)
    outs = pl.pallas_call(
        functools.partial(pair_sums, sections, (base_items, base_entries)),
        out_shape=[jax.ShapeDtypeStruct((count, 8, LEAF), jnp.float32)] * sections,
        in_specs=[smem] * 3 + [vmem] * (2 * sections),
        out_specs=[vmem] * sections,
        scratch_shapes=[
            pltpu.VMEM((blocks, 48, width), jnp.bfloat16),
            pltpu.VMEM((count, LEAF, LEAF), jnp.bfloat16),
            pltpu.VMEM((blocks, 16, width), jnp.bfloat16),
        ],
    )(src, leaves, live, *places, *channels)
    return [jnp.transpose(out, (1, 0, 2)).reshape(8, width) for out in outs]


def local(position, velocity, mass, pair_list, hot_leaf):
    pairs = pair_list[0, 0]
    hot = hot_leaf[0, 0]
    leaf_count, listed = pairs.shape
    groups = listed // base_entries
    lists = (pairs % leaf_count).reshape(leaf_count, groups, base_entries)
    alive = hot < leaf_count
    slot_leaf = jnp.minimum(hot, leaf_count - 1)
    extra_src = jnp.take(lists, slot_leaf, axis=0)[:, 1:]
    src = jnp.concatenate([lists[:, 0].reshape(-1), extra_src.reshape(-1)])
    leaves = jnp.concatenate(
        [jnp.arange(leaf_count, dtype=jnp.int32), jnp.repeat(slot_leaf, groups - 1)]
    )
    live = jnp.sum(alive.astype(jnp.int32)).reshape(1)
    tables = (src, leaves, live, leaf_count)

    centre = jnp.stack(
        [
            lax.axis_index("gx").astype(jnp.float32) + 0.5,
            lax.axis_index("gy").astype(jnp.float32) + 0.5,
            jnp.float32(0.5),
        ]
    ).reshape(1, 3, 1)
    own = blocks_own = base_entries // 2
    state = surround(jnp.concatenate([position, velocity, mass], axis=2))
    pos, vel, m = state[:, 0:3], state[:, 3:6], state[:, 6:7]
    x1 = pos - centre
    x2 = (pos + 0.5 * time_step * vel) - centre
    zeros7 = jnp.zeros((m.shape[0], 7, m.shape[2]), jnp.float32)
    mass_rows = jnp.concatenate([m, zeros7], axis=1)
    rho1, rho2 = all_sums(tables, [x1, x2], [mass_rows, mass_rows])
    own_m = mass[0, 0]
    q_own = 1.0 / (own_m + jnp.concatenate([rho1[0:1], rho2[0:1]], axis=0))
    q_all = surround(q_own[None, None])

    def acceleration(x, v, own_v, q, own_q):
        mq = m * q
        rows = jnp.concatenate([m, m * x, mq, mq * (viscosity * v - (2.0 / kernel_scale) * x)], axis=1)
        (s,) = all_sums(tables, [x], [rows])
        own_x = x[own]
        pushed = (2.0 / kernel_scale) * (
            own_q * (own_x * s[0:1] - s[1:4]) + own_x * s[4:5]
        )
        return pushed - viscosity * own_v * s[4:5] + s[5:8]

    own_v = velocity[0, 0]
    acc1 = acceleration(x1, vel, own_v, q_all[:, 0:1], q_own[0:1])
    mid_velocity = own_v + 0.5 * time_step * acc1
    mid_all = surround(mid_velocity[None, None])
    acc2 = acceleration(x2, mid_all, mid_velocity, q_all[:, 1:2], q_own[1:2])
    return (
        (time_step * mid_velocity)[None, None],
        (own_v + time_step * acc2)[None, None],
    )


def solution(mesh):
    return jax.shard_map(
        local,
        mesh=mesh,
        in_specs=(
            P("gx", "gy", None, None),
            P("gx", "gy", None, None),
            P("gx", "gy", None, None),
            P("gx", "gy", None, None),
            P("gx", "gy", None),
        ),
        out_specs=(P("gx", "gy", None, None), P("gx", "gy", None, None)),
        check_vma=False,
    )
```

```python
import functools

import jax
import jax.numpy as jnp
from jax import lax
from jax.experimental import pallas as pl
from jax.experimental.pallas import tpu as pltpu
from jax.sharding import PartitionSpec as P

LEAF = 128
MESH = pl.DeviceIdType.MESH

kernel_scale = 1.0
viscosity = 0.5
time_step = 0.5
base_entries = 9
COORD = (2.0 * 1.4426950408889634 / kernel_scale) ** 0.5


def exchange(sizes, own_ref, out_ref, send_sem, recv_sem):
    count_x, count_y = sizes
    gx, gy = lax.axis_index("gx"), lax.axis_index("gy")

    def inside(a, b):
        terms = []
        if a != 1:
            terms.append(gx > 0 if a == 0 else gx < count_x - 1)
        if b != 1:
            terms.append(gy > 0 if b == 0 else gy < count_y - 1)
        return terms[0] if len(terms) == 1 else terms[0] & terms[1]

    def device(a, b):
        return (jnp.clip(gx + a - 1, 0, count_x - 1), jnp.clip(gy + b - 1, 0, count_y - 1))

    sides = ((1, 0), (1, 2), (0, 1), (2, 1))
    barrier = pltpu.get_barrier_semaphore()
    for a, b in sides:

        @pl.when(inside(a, b))
        def _():
            pl.semaphore_signal(barrier, inc=1, device_id=device(a, b), device_id_type=MESH)

    pl.semaphore_wait(barrier, sum(inside(a, b).astype(jnp.int32) for a, b in sides))

    def copy(source, block, to):
        return pltpu.make_async_remote_copy(
            src_ref=source,
            dst_ref=out_ref.at[block],
            send_sem=send_sem.at[block],
            recv_sem=recv_sem.at[block],
            device_id=device(*to),
            device_id_type=MESH,
        )

    def sent(a, b):
        to = (1, 2 - b) if a == 1 else (2 - a, 1)
        source = own_ref if a == 1 or b == 1 else out_ref.at[3 + b]
        return copy(source, 3 * a + b, to), inside(*to) if a == 1 or b == 1 else inside(2 - a, b)

    for a, b in sides:
        descriptor, valid = sent(a, b)
        pl.when(valid)(descriptor.start)
    out_ref[4] = own_ref[...]
    for a in range(3):
        for b in range(3):
            if (a, b) != (1, 1):

                @pl.when(jnp.logical_not(inside(a, b)))
                def _():
                    out_ref[3 * a + b] = jnp.zeros(own_ref.shape, own_ref.dtype)

    for b in (0, 2):
        pl.when(inside(1, b))(sent(1, b)[0].wait_recv)
        for a in (0, 2):
            descriptor, valid = sent(a, b)
            pl.when(valid)(descriptor.start)
    for a, b in ((0, 1), (2, 1), (0, 0), (2, 0), (0, 2), (2, 2)):
        pl.when(inside(a, b))(sent(a, b)[0].wait_recv)
    for a in range(3):
        for b in range(3):
            if (a, b) != (1, 1):
                descriptor, valid = sent(a, b)
                pl.when(valid)(descriptor.wait_send)


def surround(cell, number):
    channels, width = cell.shape
    count = width // LEAF
    vmem = pl.BlockSpec(memory_space=pltpu.VMEM)
    out = pl.pallas_call(
        functools.partial(exchange, (lax.axis_size("gx"), lax.axis_size("gy"))),
        out_shape=jax.ShapeDtypeStruct((9, channels * count, LEAF), cell.dtype),
        in_specs=[vmem],
        out_specs=vmem,
        scratch_shapes=[pltpu.SemaphoreType.DMA((9,)), pltpu.SemaphoreType.DMA((9,))],
        compiler_params=pltpu.CompilerParams(collective_id=number, has_side_effects=True),
    )(cell.reshape(channels * count, LEAF))
    return out.reshape(9, channels, width)


def split3(value):
    first = value.astype(jnp.bfloat16).astype(jnp.float32)
    rest = value - first
    second = rest.astype(jnp.bfloat16).astype(jnp.float32)
    third = (rest - second).astype(jnp.bfloat16).astype(jnp.float32)
    return first, second, third


def coordinate_rows(x, ones_first):
    a = COORD * x
    c = -0.5 * jnp.sum(a * a, axis=0, keepdims=True)
    one = jnp.ones_like(c)
    pad = jnp.zeros_like(a)
    return jnp.concatenate([a, one, c, pad] if ones_first else [a, c, one, pad], axis=0)


def pair_sums(sections, counts, src_ref, leaf_ref, live_ref, *refs):
    place_refs, channel_refs = refs[:sections], refs[sections : 2 * sections]
    out_refs = refs[2 * sections : 3 * sections]
    feature, target, channel = refs[3 * sections :]
    base_items, entries = counts
    blocks, _, width = place_refs[0].shape
    step = min(width, 8 * LEAF)
    own = blocks // 2
    for place_ref, channel_ref, out_ref in zip(place_refs, channel_refs, out_refs):
        for block in range(blocks):

            def prepare(i, carry):
                span = pl.ds(pl.multiple_of(i * step, step), step)
                rows = coordinate_rows(place_ref[block, 0:3, span], True)
                s1, s2, s3 = split3(rows)
                feature[block, :, span] = jnp.concatenate(
                    [s1, s2, s1, s2, s3, s1], axis=0
                ).astype(jnp.bfloat16)
                c1, c2, _ = split3(channel_ref[block, :, span])
                channel[block, :, span] = jnp.concatenate([c1, c2], axis=0).astype(jnp.bfloat16)
                return carry

            lax.fori_loop(0, width // step, prepare, 0)

        def prepare_target(i, carry):
            span = pl.ds(pl.multiple_of(i * LEAF, LEAF), LEAF)
            rows = coordinate_rows(place_ref[own, 0:3, span], False)
            t1, t2, t3 = split3(rows)
            stack = jnp.concatenate(
                [t1, t1, t2, t2, t1, t3, jnp.zeros((LEAF - 48, LEAF), jnp.float32)], axis=0
            )
            target[i] = stack.T.astype(jnp.bfloat16)
            return carry

        lax.fori_loop(0, width // LEAF, prepare_target, 0)

        def sums(item):
            leaf = leaf_ref[item]
            spans = [
                pl.ds(pl.multiple_of(src_ref[item * entries + k] * LEAF, LEAF), LEAF)
                for k in range(entries)
            ]
            near = jnp.concatenate([feature[k, :, spans[k]] for k in range(entries)], axis=1)
            exponent = jnp.dot(
                target[leaf][:, 0:48], near, preferred_element_type=jnp.float32
            )
            weight = jnp.exp2(exponent).astype(jnp.bfloat16)
            rows = jnp.concatenate([channel[k, :, spans[k]] for k in range(entries)], axis=1)
            both = lax.dot_general(
                rows, weight, (((1,), (1,)), ((), ())), preferred_element_type=jnp.float32
            )
            return leaf, both[0:8] + both[8:16]

        def base(i, carry):
            for u in range(4):
                leaf, value = sums(i * 4 + u)
                out_ref[leaf] = value
            return carry

        lax.fori_loop(0, base_items // 4, base, 0)

        def extra(i, carry):
            leaf, first = sums(base_items + 2 * i)
            _, second = sums(base_items + 2 * i + 1)
            out_ref[leaf] = out_ref[leaf] + (first + second)
            return carry

        lax.fori_loop(0, live_ref[0], extra, 0)


def all_sums(tables, places, channels):
    src, leaves, live, base_items = tables
    sections = len(places)
    blocks, _, width = places[0].shape
    count = width // LEAF
    smem = pl.BlockSpec(memory_space=pltpu.SMEM)
    vmem = pl.BlockSpec(memory_space=pltpu.VMEM)
    outs = pl.pallas_call(
        functools.partial(pair_sums, sections, (base_items, base_entries)),
        out_shape=[jax.ShapeDtypeStruct((count, 8, LEAF), jnp.float32)] * sections,
        in_specs=[smem] * 3 + [vmem] * (2 * sections),
        out_specs=[vmem] * sections,
        scratch_shapes=[
            pltpu.VMEM((blocks, 48, width), jnp.bfloat16),
            pltpu.VMEM((count, LEAF, LEAF), jnp.bfloat16),
            pltpu.VMEM((blocks, 16, width), jnp.bfloat16),
        ],
    )(src, leaves, live, *places, *channels)
    return [jnp.transpose(out, (1, 0, 2)).reshape(8, width) for out in outs]


def local(position, velocity, mass, pair_list, hot_leaf):
    pairs = pair_list[0, 0]
    hot = hot_leaf[0, 0]
    leaf_count, listed = pairs.shape
    groups = listed // base_entries
    lists = (pairs % leaf_count).reshape(leaf_count, groups, base_entries)
    alive = hot < leaf_count
    slot_leaf = jnp.minimum(hot, leaf_count - 1)
    extra_src = jnp.take(lists, slot_leaf, axis=0)[:, 1:]
    src = jnp.concatenate([lists[:, 0].reshape(-1), extra_src.reshape(-1)])
    leaves = jnp.concatenate(
        [jnp.arange(leaf_count, dtype=jnp.int32), jnp.repeat(slot_leaf, groups - 1)]
    )
    live = jnp.sum(alive.astype(jnp.int32)).reshape(1)
    tables = (src, leaves, live, leaf_count)

    centre = jnp.stack(
        [
            lax.axis_index("gx").astype(jnp.float32) + 0.5,
            lax.axis_index("gy").astype(jnp.float32) + 0.5,
            jnp.float32(0.5),
        ]
    ).reshape(1, 3, 1)
    own = base_entries // 2
    state = surround(jnp.concatenate([position, velocity, mass], axis=2)[0, 0], 0)
    pos, vel, m = state[:, 0:3], state[:, 3:6], state[:, 6:7]
    x1 = pos - centre
    x2 = (pos + 0.5 * time_step * vel) - centre
    zeros7 = jnp.zeros((m.shape[0], 7, m.shape[2]), jnp.float32)
    mass_rows = jnp.concatenate([m, zeros7], axis=1)
    rho1, rho2 = all_sums(tables, [x1, x2], [mass_rows, mass_rows])
    own_m = mass[0, 0]
    q_own = 1.0 / (own_m + jnp.concatenate([rho1[0:1], rho2[0:1]], axis=0))
    q_all = surround(q_own, 1)

    def acceleration(x, v, own_v, q, own_q):
        mq = m * q
        rows = jnp.concatenate([m, m * x, mq, mq * (viscosity * v - (2.0 / kernel_scale) * x)], axis=1)
        (s,) = all_sums(tables, [x], [rows])
        own_x = x[own]
        pushed = (2.0 / kernel_scale) * (
            own_q * (own_x * s[0:1] - s[1:4]) + own_x * s[4:5]
        )
        return pushed - viscosity * own_v * s[4:5] + s[5:8]

    own_v = velocity[0, 0]
    acc1 = acceleration(x1, vel, own_v, q_all[:, 0:1], q_own[0:1])
    mid_velocity = own_v + 0.5 * time_step * acc1
    mid_all = surround(mid_velocity, 2)
    acc2 = acceleration(x2, mid_all, mid_velocity, q_all[:, 1:2], q_own[1:2])
    return (
        (time_step * mid_velocity)[None, None],
        (own_v + time_step * acc2)[None, None],
    )


def solution(mesh):
    return jax.shard_map(
        local,
        mesh=mesh,
        in_specs=(
            P("gx", "gy", None, None),
            P("gx", "gy", None, None),
            P("gx", "gy", None, None),
            P("gx", "gy", None, None),
            P("gx", "gy", None),
        ),
        out_specs=(P("gx", "gy", None, None), P("gx", "gy", None, None)),
        check_vma=False,
    )
```
